16 devices in a mesh: dp: 2 (over z), ep: 8 (over y, x, core).
Axes of the slice: x: 2, y: 2, z: 2, core: 2. Of those that a mesh axis runs over, the one named last changes fastest.
Arguments:
- x_tokens: bfloat16 [131072, 768], P(('dp', 'ep'))
- expert_id: int32 [131072], P(('dp', 'ep'))
- token_slot: int32 [131072], P(('dp', 'ep'))
- grad_y: bfloat16 [131072, 768], P(('dp', 'ep'))
- w_router: float32 [768, 32], replicated
- w_in: bfloat16 [32, 768, 3072], P('ep')
- w_out: bfloat16 [32, 3072, 768], P('ep')
- row_in: float32 [32, 768], P('ep')
- col_in: float32 [32, 3072], P('ep')
- row_out: float32 [32, 3072], P('ep')
- col_out: float32 [32, 768], P('ep')
- row_router: float32 [768], replicated
- col_router: float32 [32], replicated
Outputs:
- output 1: bfloat16 [32, 768, 3072], P('ep')
- output 2: bfloat16 [32, 3072, 768], P('ep')
- output 3: float32 [768, 32], replicated
- output 4: float32 [32, 768], P('ep')
- output 5: float32 [32, 3072], P('ep')
- output 6: float32 [32, 3072], P('ep')
- output 7: float32 [32, 768], P('ep')
- output 8: float32 [768], replicated
- output 9: float32 [32], replicated
- output 10: bfloat16 [131072, 768], P(('dp', 'ep'))
All inputs are finite; a program needn't handle non-finite values.
Results may differ from the reference program's by a relative error of at most 0.00322.
Values are sent between devices in bfloat16 or wider.
A program may use at most 1 GiB of HBM per device.

```python
import jax
import jax.numpy as jnp
from jax import lax
import math

GROUPS = 16
TOK = 8192
D = 768
FF = 3072
E = 32
CAPACITY = 320
OPT_STEP = 2

DECAY_RATE = 1.0 - OPT_STEP ** -0.8
LR_BASE = min(0.01, 1.0 / math.sqrt(OPT_STEP))
AUX_COEF = 0.01
PRECISE = lax.Precision.HIGHEST


def draw_routing(base_key):
    key_hot, key_shift, key_rand = jax.random.split(base_key, 3)
    hot_id = jax.random.randint(key_hot, (GROUPS, 1), 0, E)
    shift_id = jax.random.randint(key_shift, (GROUPS, 1), 0, E)
    rand_ids = jax.random.randint(key_rand, (GROUPS, TOK), 0, E)
    position = jnp.arange(TOK)[None, :]
    spread = (position // 4 + shift_id) % E
    spread_row = (position % 4 == 1) & (position // 4 < E)
    expert_id = jnp.where(position % 4 == 0, hot_id, jnp.where(spread_row, spread, rand_ids))
    onehot = (expert_id[:, :, None] == jnp.arange(E)[None, None, :]).astype(jnp.int32)
    arrive_rank = jnp.sum(jnp.cumsum(onehot, axis=1) * onehot, axis=2) - 1
    token_slot = jnp.where(arrive_rank < CAPACITY, arrive_rank, -1)
    return expert_id.reshape(GROUPS * TOK).astype(jnp.int32), token_slot.reshape(GROUPS * TOK).astype(jnp.int32)


def draw_stat(stat_key, stat_shape, stat_scale):
    return stat_scale * jnp.exp(jax.random.uniform(stat_key, stat_shape, jnp.float32, -1.0, 1.0))


def setup_inputs(seed: int = 0) -> dict:
    sub_keys = jax.random.split(jax.random.key(seed), 12)
    all_tokens = GROUPS * TOK
    x_tokens = jax.random.normal(sub_keys[0], (all_tokens, D), jnp.float32).astype(jnp.bfloat16)
    grad_y = jax.random.normal(sub_keys[1], (all_tokens, D), jnp.float32).astype(jnp.bfloat16)
    expert_id, token_slot = draw_routing(sub_keys[2])
    w_router = jax.random.normal(sub_keys[3], (D, E), jnp.float32) * D ** -0.5
    w_in = (jax.random.normal(sub_keys[4], (E, D, FF), jnp.float32) * D ** -0.5).astype(jnp.bfloat16)
    w_out = (jax.random.normal(sub_keys[5], (E, FF, D), jnp.float32) * FF ** -0.5).astype(jnp.bfloat16)
    out_scale = 1.36 * GROUPS * TOK / E ** 3
    in_scale = out_scale * D / FF
    router_scale = out_scale * D
    return dict(x_tokens=x_tokens, expert_id=expert_id, token_slot=token_slot, grad_y=grad_y, w_router=w_router, w_in=w_in, w_out=w_out, row_in=draw_stat(sub_keys[6], (E, D), in_scale), col_in=draw_stat(sub_keys[7], (E, FF), in_scale), row_out=draw_stat(sub_keys[8], (E, FF), out_scale), col_out=draw_stat(sub_keys[9], (E, D), out_scale), row_router=draw_stat(sub_keys[10], (D,), router_scale), col_router=draw_stat(sub_keys[11], (E,), router_scale))


def gather_rows(table, index):
    return jax.vmap(lambda group_rows, group_index: jnp.take(group_rows, group_index, axis=0, mode='fill', fill_value=0))(table, index)


def slot_sources(flat_pos):
    return jnp.full((E * CAPACITY,), TOK, jnp.int32).at[flat_pos].set(jnp.arange(TOK, dtype=jnp.int32), mode='drop')


def optimizer_step(weight, gradient, row_stat, col_stat):
    grad_sq = gradient * gradient + 1e-30
    row_new = DECAY_RATE * row_stat + (1.0 - DECAY_RATE) * jnp.mean(grad_sq, axis=-1)
    col_new = DECAY_RATE * col_stat + (1.0 - DECAY_RATE) * jnp.mean(grad_sq, axis=-2)
    row_norm = row_new / jnp.mean(row_new, axis=-1, keepdims=True)
    update = gradient * lax.rsqrt(row_norm)[..., :, None] * lax.rsqrt(col_new)[..., None, :]
    upd_rms = jnp.sqrt(jnp.mean(update * update, axis=(-2, -1), keepdims=True))
    update = update / jnp.maximum(1.0, upd_rms)
    w_full = weight.astype(jnp.float32)
    w_rms = jnp.sqrt(jnp.mean(w_full * w_full, axis=(-2, -1), keepdims=True))
    new_weight = w_full - LR_BASE * jnp.maximum(1e-3, w_rms) * update
    return new_weight, row_new, col_new


def expert_step(operands):
    buf_x, buf_gh, win_e, wout_e = operands
    win_f = win_e.astype(jnp.float32)
    wout_f = wout_e.astype(jnp.float32)
    pre_act = jnp.einsum('gcd,df->gcf', buf_x.astype(jnp.float32), win_f).astype(jnp.bfloat16)
    hid_act = jnp.maximum(pre_act, 0)
    exp_out = jnp.einsum('gcf,fd->gcd', hid_act.astype(jnp.float32), wout_f).astype(jnp.bfloat16)
    grad_act = jnp.einsum('gcd,fd->gcf', buf_gh.astype(jnp.float32), wout_f)
    grad_pre = jnp.where(pre_act > 0, grad_act, 0.0).astype(jnp.bfloat16)
    grad_wout = jnp.einsum('gcf,gcd->fd', hid_act.astype(jnp.float32), buf_gh.astype(jnp.float32))
    grad_win = jnp.einsum('gcd,gcf->df', buf_x.astype(jnp.float32), grad_pre.astype(jnp.float32))
    grad_buf = jnp.einsum('gcf,df->gcd', grad_pre.astype(jnp.float32), win_f).astype(jnp.bfloat16)
    return exp_out, grad_buf, grad_win, grad_wout


def reference(x_tokens, expert_id, token_slot, grad_y, w_router, w_in, w_out, row_in, col_in, row_out, col_out, row_router, col_router):
    x_grp = x_tokens.reshape(GROUPS, TOK, D)
    dy_grp = grad_y.reshape(GROUPS, TOK, D)
    group_ids = expert_id.reshape(GROUPS, TOK)
    group_slots = token_slot.reshape(GROUPS, TOK)
    x_wide = x_grp.astype(jnp.float32)
    logits = jnp.einsum('gtd,de->gte', x_wide, w_router, precision=PRECISE)
    gate_probs = jax.nn.softmax(logits, axis=-1)
    onehot = (group_ids[:, :, None] == jnp.arange(E)[None, None, :]).astype(jnp.float32)
    gate_val = jnp.sum(gate_probs * onehot, axis=-1)
    flat_pos = jnp.where(group_slots >= 0, group_ids * CAPACITY + group_slots, E * CAPACITY)
    src_tok = jax.vmap(slot_sources)(flat_pos)
    send_x = gather_rows(x_grp, src_tok).reshape(GROUPS, E, CAPACITY, D)
    grad_h = (gate_val[:, :, None] * dy_grp.astype(jnp.float32)).astype(jnp.bfloat16)
    send_gh = gather_rows(grad_h, src_tok).reshape(GROUPS, E, CAPACITY, D)
    exp_out, grad_buf, grad_win, grad_wout = lax.map(expert_step, (jnp.swapaxes(send_x, 0, 1), jnp.swapaxes(send_gh, 0, 1), w_in, w_out))
    out_tok = gather_rows(jnp.swapaxes(exp_out, 0, 1).reshape(GROUPS, E * CAPACITY, D), flat_pos)
    dx_expert = gather_rows(jnp.swapaxes(grad_buf, 0, 1).reshape(GROUPS, E * CAPACITY, D), flat_pos)
    grad_gate = jnp.sum(dy_grp.astype(jnp.float32) * out_tok.astype(jnp.float32), axis=-1)
    route_frac = jnp.mean(onehot, axis=1, keepdims=True)
    grad_prob = onehot * grad_gate[:, :, None] + AUX_COEF * E * route_frac / TOK
    grad_logits = gate_probs * (grad_prob - jnp.sum(gate_probs * grad_prob, axis=-1, keepdims=True))
    grad_router = jnp.einsum('gtd,gte->de', x_wide, grad_logits, precision=PRECISE)
    grad_x = (dx_expert.astype(jnp.float32) + jnp.einsum('gte,de->gtd', grad_logits, w_router, precision=PRECISE)).astype(jnp.bfloat16)
    new_in, row_in_new, col_in_new = optimizer_step(w_in, grad_win, row_in, col_in)
    new_out, row_out_new, col_out_new = optimizer_step(w_out, grad_wout, row_out, col_out)
    new_router, row_router_new, col_router_new = optimizer_step(w_router, grad_router, row_router, col_router)
    return (new_in.astype(jnp.bfloat16), new_out.astype(jnp.bfloat16), new_router, row_in_new, col_in_new, row_out_new, col_out_new, row_router_new, col_router_new, grad_x.reshape(GROUPS * TOK, D))
```

```python
import jax
import jax.numpy as jnp
from jax import lax
from jax.sharding import PartitionSpec as P
import math

OPT_STEP = 2
DECAY_RATE = 1.0 - OPT_STEP ** -0.8
LR_BASE = min(0.01, 1.0 / math.sqrt(OPT_STEP))
AUX_COEF = 0.01
PRECISE = lax.Precision.HIGHEST
F32 = jnp.float32
BF16 = jnp.bfloat16


def optimizer_step(weight, gradient, row_stat, col_stat):
    grad_sq = gradient * gradient + 1e-30
    row_new = DECAY_RATE * row_stat + (1.0 - DECAY_RATE) * jnp.mean(grad_sq, axis=-1)
    col_new = DECAY_RATE * col_stat + (1.0 - DECAY_RATE) * jnp.mean(grad_sq, axis=-2)
    row_norm = row_new / jnp.mean(row_new, axis=-1, keepdims=True)
    update = gradient * lax.rsqrt(row_norm)[..., :, None] * lax.rsqrt(col_new)[..., None, :]
    upd_rms = jnp.sqrt(jnp.mean(update * update, axis=(-2, -1), keepdims=True))
    update = update / jnp.maximum(1.0, upd_rms)
    w_full = weight.astype(F32)
    w_rms = jnp.sqrt(jnp.mean(w_full * w_full, axis=(-2, -1), keepdims=True))
    new_weight = w_full - LR_BASE * jnp.maximum(1e-3, w_rms) * update
    return new_weight, row_new, col_new


def split3(value):
    hi = lax.reduce_precision(value, 8, 7)
    rest = value - hi
    mid = lax.reduce_precision(rest, 8, 7)
    lo = rest - mid
    return hi.astype(BF16), mid.astype(BF16), lo.astype(BF16)


def mm(a, b, dims):
    return lax.dot_general(a, b, (dims, ((), ())), preferred_element_type=F32)


def solution(mesh):
    ep_size = mesh.shape['ep']
    dp_size = mesh.shape['dp']
    tok_spec = P(('dp', 'ep'))
    row_spec = P(('dp', 'ep'), None)
    exp_spec = P('ep')
    full_spec = P()
    swap = [(i, (i + 1) % dp_size) for i in range(dp_size)]

    def local_step(x_tokens, expert_id, token_slot, grad_y, w_router, w_in, w_out, row_in, col_in, row_out, col_out, row_router, col_router):
        tokens, width = x_tokens.shape
        el = w_in.shape[0]
        experts = w_router.shape[1]
        cap = 5 * tokens // (4 * experts)
        own = el // dp_size
        zi = lax.axis_index('dp')
        base = own * zi

        is_e = expert_id[:, None] == jnp.arange(experts)[None, :]
        onehot = is_e.astype(F32)
        onehot_b = is_e.astype(BF16)
        is_c = token_slot[:, None] == jnp.arange(cap)[None, :]
        tok_idx = jnp.arange(tokens, dtype=jnp.int32)

        def to_slots(vals):
            cols = jnp.concatenate([jnp.where(is_c, v.astype(BF16)[:, None], jnp.zeros((), BF16)) for v in vals], axis=1)
            out = mm(onehot_b, cols, ((0,), (0,)))
            return [out[:, i * cap:(i + 1) * cap] for i in range(len(vals))]

        t_hi, t_lo, t_cnt = to_slots([tok_idx // 64, tok_idx % 64, jnp.ones_like(tok_idx)])
        src = (t_hi * 64.0 + t_lo).astype(jnp.int32)
        src = jnp.where(t_cnt > 0.5, src, tokens)

        def by_pos(table):
            return jnp.roll(table.reshape(ep_size, el, cap), -base, axis=1)

        src_pos = by_pos(src)

        r_hi, r_mid, r_lo = split3(w_router)
        lg = mm(x_tokens, jnp.concatenate([r_hi, r_mid, r_lo], axis=1), ((1,), (0,)))
        logits = lg[:, :experts] + (lg[:, experts:2 * experts] + lg[:, 2 * experts:])
        gate_probs = jax.nn.softmax(logits, axis=-1)
        gate_val = jnp.sum(gate_probs * onehot, axis=-1)
        p_hi, p_mid, p_lo = to_slots(list(split3(gate_val)))
        p_slot = p_hi + (p_mid + p_lo)
        p_recv = lax.all_to_all(by_pos(p_slot), 'ep', 0, 0, tiled=True)

        def send(rows, q):
            buf = jnp.take(rows, src_pos[:, q].reshape(-1), axis=0, mode='fill', fill_value=0)
            buf = buf.reshape(ep_size, cap, width)
            return lax.all_to_all(buf, 'ep', 0, 0, tiled=True).reshape(ep_size * cap, width)

        def weight(w, q):
            return lax.dynamic_index_in_dim(w, lax.rem(base + q, el), 0, keepdims=False)

        order = []
        for k in range(own):
            order += [own + k, k]
        res = {}
        g_pos, back = {}, {}
        for q in order:
            xq = send(x_tokens, q)
            yq = send(grad_y, q)
            w1, w2 = weight(w_in, q), weight(w_out, q)
            pq = p_recv[:, q].reshape(-1)
            dhq = (pq[:, None] * yq).astype(BF16)
            pre = mm(xq, w1, ((1,), (0,))).astype(BF16)
            act = jnp.maximum(pre, 0)
            h = mm(act, w2, ((1,), (0,))).astype(BF16)
            g_pos[q] = jnp.sum(yq.astype(F32) * h.astype(F32), axis=-1)
            da = jnp.where(pre > 0, mm(dhq, w2, ((1,), (1,))), 0.0).astype(BF16)
            dbuf = mm(da, w1, ((1,), (1,))).astype(BF16)
            back[q] = lax.all_to_all(dbuf.reshape(ep_size, cap, width), 'ep', 0, 0, tiled=True).reshape(ep_size * cap, width)
            res[q] = (xq, dhq, act, da)

        new_in, new_out, stats = [], [], []
        for k in range(own):
            w1, w2 = weight(w_in, k), weight(w_out, k)
            xp = lax.ppermute(res[own + k][0], 'dp', swap)
            dhp = lax.ppermute(res[own + k][1], 'dp', swap)
            pre_p = mm(xp, w1, ((1,), (0,))).astype(BF16)
            act_p = jnp.maximum(pre_p, 0)
            da_p = jnp.where(pre_p > 0, mm(dhp, w2, ((1,), (1,))), 0.0).astype(BF16)
            xq, dhq, act, da = res[k]
            d_out = mm(act, dhq, ((0,), (0,))) + mm(act_p, dhp, ((0,), (0,)))
            d_in = mm(xq, da, ((0,), (0,))) + mm(xp, da_p, ((0,), (0,)))
            no, ro, co = optimizer_step(w2, d_out, weight(row_out, k), weight(col_out, k))
            ni, ri, ci = optimizer_step(w1, d_in, weight(row_in, k), weight(col_in, k))
            new_out.append(no.astype(BF16))
            new_in.append(ni.astype(BF16))
            stats.append((ri, ci, ro, co))

        def assemble(mine, like):
            theirs = [lax.ppermute(m, 'dp', swap) for m in mine]
            out = jnp.zeros((el,) + mine[0].shape, like)
            for k, m in enumerate(mine):
                out = lax.dynamic_update_index_in_dim(out, m, lax.rem(base + k, el), 0)
            for k, m in enumerate(theirs):
                out = lax.dynamic_update_index_in_dim(out, m, lax.rem(base + own + k, el), 0)
            return out

        out_w_out = assemble(new_out, BF16)
        out_w_in = assemble(new_in, BF16)
        out_stats = []
        for i in range(4):
            mine = jnp.stack([s[i] for s in stats])
            both = jnp.concatenate([mine, lax.ppermute(mine, 'dp', swap)], axis=0)
            out_stats.append(jnp.roll(both, base, axis=0))

        g_buf = jnp.stack([g_pos[q].reshape(ep_size, cap) for q in range(el)], axis=1)
        g_back = lax.all_to_all(g_buf, 'ep', 0, 0, tiled=True)
        g_slot = jnp.roll(g_back, base, axis=1).reshape(experts, cap)
        g3 = jnp.concatenate(split3(g_slot), axis=0)
        onehot3 = jnp.concatenate([onehot_b] * 3, axis=1)
        g_rows = mm(onehot3, g3, ((1,), (0,)))
        grad_gate = jnp.sum(jnp.where(is_c, g_rows, 0.0), axis=-1)

        route_frac = jnp.mean(onehot, axis=0)
        grad_prob = onehot * grad_gate[:, None] + AUX_COEF * experts * route_frac[None, :] / tokens
        grad_logits = gate_probs * (grad_prob - jnp.sum(gate_probs * grad_prob, axis=-1, keepdims=True))
        l1, l2, l3 = split3(grad_logits)
        gr = mm(x_tokens, jnp.concatenate([l1, l2, l3], axis=1), ((0,), (0,)))
        grad_router = lax.psum(gr[:, :experts] + (gr[:, experts:2 * experts] + gr[:, 2 * experts:]), ('dp', 'ep'))
        lcat = jnp.concatenate([l1, l1, l2, l1, l2, l3], axis=1)
        wcat = jnp.concatenate([r_hi, r_mid, r_hi, r_lo, r_mid, r_hi], axis=1)
        dx_router = mm(lcat, wcat, ((1,), (1,)))

        back_all = jnp.concatenate([back[q] for q in range(el)], axis=0)
        pos_e = lax.rem(expert_id % el - base + el, el)
        back_pos = jnp.where(token_slot >= 0, (pos_e * ep_size + expert_id // el) * cap + token_slot, experts * cap)
        dx_expert = jnp.take(back_all, back_pos, axis=0, mode='fill', fill_value=0)
        grad_x = (dx_expert.astype(F32) + dx_router).astype(BF16)
        new_router, row_router_new, col_router_new = optimizer_step(w_router, grad_router, row_router, col_router)
        return (out_w_in, out_w_out, new_router, out_stats[0], out_stats[1], out_stats[2], out_stats[3], row_router_new, col_router_new, grad_x)

    in_specs = (row_spec, tok_spec, tok_spec, row_spec, full_spec, exp_spec, exp_spec, exp_spec, exp_spec, exp_spec, exp_spec, full_spec, full_spec)
    out_specs = (exp_spec, exp_spec, full_spec, exp_spec, exp_spec, exp_spec, exp_spec, full_spec, full_spec, row_spec)
    return jax.shard_map(local_step, mesh=mesh, in_specs=in_specs, out_specs=out_specs, check_vma=False)
```

```python
import functools
import math

import jax
import jax.numpy as jnp
from jax import lax
from jax.experimental import pallas as pl
from jax.experimental.pallas import tpu as pltpu
from jax.sharding import PartitionSpec as P

OPT_STEP = 2
DECAY_RATE = 1.0 - OPT_STEP ** -0.8
LR_BASE = min(0.01, 1.0 / math.sqrt(OPT_STEP))
AUX_COEF = 0.01
F32 = jnp.float32
BF16 = jnp.bfloat16
ROW_BLOCK = 640
F_CHUNK = 512
G_CHUNK = 64


def kdot(a, b, ca, cb):
    return lax.dot_general(a, b, (((ca,), (cb,)), ((), ())), preferred_element_type=F32)


def adafactor_tile(acc, sub_old, lane_old, sub_new_ref, lane_new_ref, lane_sum, row_is_sub):
    rows, cols = acc.shape
    lane_sum[...] = jnp.zeros_like(lane_sum)

    @pl.loop(0, rows // G_CHUNK)
    def _(i):
        at = pl.ds(pl.multiple_of(i * G_CHUNK, G_CHUNK), G_CHUNK)
        g = acc[at, :]
        v = g * g + 1e-30
        sub_new_ref[at, :] = DECAY_RATE * sub_old[at, :] + (1.0 - DECAY_RATE) * (jnp.sum(v, axis=1, keepdims=True) * (1.0 / cols))
        lane_sum[...] += jnp.sum(v.reshape(G_CHUNK // 8, 8, cols), axis=0)

    lane_new = DECAY_RATE * lane_old[...] + (1.0 - DECAY_RATE) * (jnp.sum(lane_sum[...], axis=0, keepdims=True) * (1.0 / rows))
    lane_new_ref[...] = lane_new
    sub_new = sub_new_ref[...]
    if row_is_sub:
        sub_f = lax.rsqrt(sub_new / (jnp.sum(sub_new, axis=0, keepdims=True) * (1.0 / rows)))
        lane_f = lax.rsqrt(lane_new)
    else:
        lane_f = lax.rsqrt(lane_new / (jnp.sum(lane_new, axis=1, keepdims=True) * (1.0 / cols)))
        sub_f = lax.rsqrt(sub_new)
    return sub_f, lane_f


def expert_kernel(opt, own_blocks, ids, *refs):
    if opt:
        (x_own, y_own, p_own, x_par, y_par, p_par, w_in, w_out, sub_in, lane_in, sub_out, lane_out, full_in_i, full_out_i,
         dbuf, g_out, new_in, new_out, full_in, full_out, sub_in_n, lane_in_n, sub_out_n, lane_out_n,
         w1, w2, sems, h_acc, b_acc, acc_in, acc_out, sub_f, lane_sum) = refs
    else:
        (x_own, y_own, p_own, w_in, w_out, dbuf, g_out, w1, w2, sems, h_acc, b_acc) = refs
    step = pl.program_id(0)
    width, ff = w1.shape
    chunks = ff // F_CHUNK

    @pl.when(step == 0)
    def _():
        c1 = pltpu.make_async_copy(w_in.at[ids[0]], w1, sems.at[0])
        c2 = pltpu.make_async_copy(w_out.at[ids[0]], w2, sems.at[1])
        c1.start()
        c2.start()
        c1.wait()
        c2.wait()
        if opt:
            acc_in[...] = jnp.zeros_like(acc_in)
            acc_out[...] = jnp.zeros_like(acc_out)

    def body(x_ref, y_ref, p_ref, own):
        x = x_ref[...]
        y = y_ref[...].astype(F32)
        dh = (p_ref[...] * y).astype(BF16)
        if opt:
            x_t = x.T
            dh_t = dh.T
        if own:
            h_acc[...] = jnp.zeros_like(h_acc)
            b_acc[...] = jnp.zeros_like(b_acc)

        @pl.loop(0, chunks)
        def _(c):
            at = pl.ds(pl.multiple_of(c * F_CHUNK, F_CHUNK), F_CHUNK)
            w1c = w1[:, at]
            w2c = w2[at, :]
            act = jnp.maximum(kdot(x, w1c, 1, 0).astype(BF16), 0)
            ga = kdot(dh, w2c, 1, 1)
            da = jnp.where(act.astype(F32) > 0, ga, 0.0).astype(BF16)
            if own:
                h_acc[...] += kdot(act, w2c, 1, 0)
                b_acc[...] += kdot(da, w1c, 1, 1)
            if opt:
                acc_in[:, at] += kdot(x_t, da, 1, 0)
                acc_out[:, at] += kdot(dh_t, act, 1, 0)

        if own:
            h = h_acc[...].astype(BF16).astype(F32)
            g_out[...] = jnp.sum(y_ref[...].astype(F32) * h, axis=1, keepdims=True)
            dbuf[...] = b_acc[...].astype(BF16)

    if opt:
        @pl.when(step < own_blocks)
        def _():
            body(x_own, y_own, p_own, True)

        @pl.when(step >= own_blocks)
        def _():
            body(x_par, y_par, p_par, False)

        @pl.when(step == pl.num_programs(0) - 1)
        def _():
            n = float(width * ff)

            def w_scale(w):
                rows = w.shape[0]

                def one(i, tot):
                    t = w[pl.ds(pl.multiple_of(i * G_CHUNK, G_CHUNK), G_CHUNK), :].astype(F32)
                    return tot + jnp.sum(jnp.sum(t * t, axis=1, keepdims=True), axis=0, keepdims=True)
                tot = lax.fori_loop(0, rows // G_CHUNK, one, jnp.zeros((1, 1), F32))
                return LR_BASE * jnp.maximum(1e-3, jnp.sqrt(tot * (1.0 / n)))

            def u_scale(acc, lane_f):
                def one(i, tot):
                    at = pl.ds(pl.multiple_of(i * G_CHUNK, G_CHUNK), G_CHUNK)
                    u = acc[at, :] * sub_f[at, :] * lane_f
                    acc[at, :] = u
                    return tot + jnp.sum(jnp.sum(u * u, axis=1, keepdims=True), axis=0, keepdims=True)
                tot = lax.fori_loop(0, width // G_CHUNK, one, jnp.zeros((1, 1), F32))
                return 1.0 / jnp.maximum(1.0, jnp.sqrt(tot * (1.0 / n)))

            sf, lf = adafactor_tile(acc_in, sub_in, lane_in, sub_in_n, lane_in_n, lane_sum, True)
            sub_f[...] = sf
            scale = u_scale(acc_in, lf) * w_scale(w1)

            @pl.loop(0, width // G_CHUNK)
            def _(i):
                at = pl.ds(pl.multiple_of(i * G_CHUNK, G_CHUNK), G_CHUNK)
                w1[at, :] = (w1[at, :].astype(F32) - scale * acc_in[at, :]).astype(BF16)

            o1 = pltpu.make_async_copy(w1, new_in, sems.at[0])
            o2 = pltpu.make_async_copy(w1, full_in.at[ids[0]], sems.at[1])
            o1.start()
            o2.start()

            sf2, lf2 = adafactor_tile(acc_out, sub_out, lane_out, sub_out_n, lane_out_n, lane_sum, False)
            sub_f[...] = sf2
            scale2 = u_scale(acc_out, lf2) * w_scale(w2)
            tc = 256

            @pl.loop(0, ff // tc)
            def _(i):
                at = pl.ds(pl.multiple_of(i * tc, tc), tc)
                w2[at, :] = (w2[at, :].astype(F32) - scale2 * acc_out[:, at].T).astype(BF16)

            o3 = pltpu.make_async_copy(w2, new_out, sems.at[2])
            o4 = pltpu.make_async_copy(w2, full_out.at[ids[0]], sems.at[3])
            o3.start()
            o4.start()
            o1.wait()
            o2.wait()
            o3.wait()
            o4.wait()
    else:
        body(x_own, y_own, p_own, True)


def expert_call(eid, x, y, p, w_in, w_out, partner=None, stats=None, full=None):
    opt = partner is not None
    rows, width = x.shape
    el, _, ff = w_in.shape
    nb = rows // ROW_BLOCK
    steps = 2 * nb if opt else nb
    own_map = lambda i, ids: (jnp.minimum(i, nb - 1), 0)
    par_map = lambda i, ids: (jnp.maximum(i - nb, 0), 0)
    fixed = lambda i, ids: (0, 0)
    any_spec = pl.BlockSpec(memory_space=pl.ANY)

    def row_specs(m):
        return [pl.BlockSpec((ROW_BLOCK, width), m), pl.BlockSpec((ROW_BLOCK, width), m), pl.BlockSpec((ROW_BLOCK, 1), m)]

    in_specs = row_specs(own_map)
    args = [x, y, p]
    if opt:
        in_specs += row_specs(par_map)
        args += list(partner)
    in_specs += [any_spec, any_spec]
    args += [w_in, w_out]
    out_shape = [jax.ShapeDtypeStruct((rows, width), BF16), jax.ShapeDtypeStruct((rows, 1), F32)]
    out_specs = [pl.BlockSpec((ROW_BLOCK, width), own_map), pl.BlockSpec((ROW_BLOCK, 1), own_map)]
    scratch = [pltpu.VMEM((width, ff), BF16), pltpu.VMEM((ff, width), BF16), pltpu.SemaphoreType.DMA((4,)),
               pltpu.VMEM((ROW_BLOCK, width), F32), pltpu.VMEM((ROW_BLOCK, width), F32)]
    aliases = {}
    units = 4
    if opt:
        units = 10
        sub = pl.BlockSpec((width, 1), fixed)
        lane = pl.BlockSpec((1, ff), fixed)
        in_specs += [sub, lane, sub, lane, any_spec, any_spec]
        args += list(stats)
        if full is None:
            full = (jnp.zeros((8, 128), BF16), jnp.zeros((8, 128), BF16))
        else:
            aliases = {1 + len(args): 4, 2 + len(args): 5}
        args += list(full)
        s, l = jax.ShapeDtypeStruct((width, 1), F32), jax.ShapeDtypeStruct((1, ff), F32)
        out_shape += [jax.ShapeDtypeStruct((width, ff), BF16), jax.ShapeDtypeStruct((ff, width), BF16),
                      jax.ShapeDtypeStruct(w_in.shape, BF16), jax.ShapeDtypeStruct(w_out.shape, BF16), s, l, s, l]
        out_specs += [any_spec] * 4 + [sub, lane, sub, lane]
        scratch += [pltpu.VMEM((width, ff), F32), pltpu.VMEM((width, ff), F32), pltpu.VMEM((width, 1), F32), pltpu.VMEM((8, ff), F32)]
    return pl.pallas_call(
        functools.partial(expert_kernel, opt, nb),
        grid_spec=pltpu.PrefetchScalarGridSpec(num_scalar_prefetch=1, grid=(steps,), in_specs=in_specs, out_specs=out_specs, scratch_shapes=scratch),
        out_shape=out_shape,
        input_output_aliases=aliases,
        compiler_params=pltpu.CompilerParams(dimension_semantics=('arbitrary',), vmem_limit_bytes=64_000_000),
        cost_estimate=pl.CostEstimate(flops=units * 2 * rows * width * ff, bytes_accessed=4 * rows * width * 2 + 4 * width * ff, transcendentals=0),
        name='expert_opt' if opt else 'expert_rows',
    )(eid, *args)


def optimizer_step(weight, gradient, row_stat, col_stat):
    grad_sq = gradient * gradient + 1e-30
    row_new = DECAY_RATE * row_stat + (1.0 - DECAY_RATE) * jnp.mean(grad_sq, axis=-1)
    col_new = DECAY_RATE * col_stat + (1.0 - DECAY_RATE) * jnp.mean(grad_sq, axis=-2)
    row_norm = row_new / jnp.mean(row_new, axis=-1, keepdims=True)
    update = gradient * lax.rsqrt(row_norm)[..., :, None] * lax.rsqrt(col_new)[..., None, :]
    upd_rms = jnp.sqrt(jnp.mean(update * update, axis=(-2, -1), keepdims=True))
    update = update / jnp.maximum(1.0, upd_rms)
    w_full = weight.astype(F32)
    w_rms = jnp.sqrt(jnp.mean(w_full * w_full, axis=(-2, -1), keepdims=True))
    new_weight = w_full - LR_BASE * jnp.maximum(1e-3, w_rms) * update
    return new_weight, row_new, col_new


def split3(value):
    hi = lax.reduce_precision(value, 8, 7)
    rest = value - hi
    mid = lax.reduce_precision(rest, 8, 7)
    lo = rest - mid
    return hi.astype(BF16), mid.astype(BF16), lo.astype(BF16)


def mm(a, b, dims):
    return lax.dot_general(a, b, (dims, ((), ())), preferred_element_type=F32)


def solution(mesh):
    ep_size = mesh.shape['ep']
    dp_size = mesh.shape['dp']
    tok_spec = P(('dp', 'ep'))
    row_spec = P(('dp', 'ep'), None)
    exp_spec = P('ep')
    full_spec = P()
    swap = [(i, (i + 1) % dp_size) for i in range(dp_size)]

    def local_step(x_tokens, expert_id, token_slot, grad_y, w_router, w_in, w_out, row_in, col_in, row_out, col_out, row_router, col_router):
        tokens, width = x_tokens.shape
        el = w_in.shape[0]
        experts = w_router.shape[1]
        cap = 5 * tokens // (4 * experts)
        own = el // dp_size
        zi = lax.axis_index('dp')
        base = own * zi

        is_e = expert_id[:, None] == jnp.arange(experts)[None, :]
        onehot = is_e.astype(F32)
        onehot_b = is_e.astype(BF16)
        is_c = token_slot[:, None] == jnp.arange(cap)[None, :]
        tok_idx = jnp.arange(tokens, dtype=jnp.int32)

        def to_slots(vals):
            cols = jnp.concatenate([jnp.where(is_c, v.astype(BF16)[:, None], jnp.zeros((), BF16)) for v in vals], axis=1)
            out = mm(onehot_b, cols, ((0,), (0,)))
            return [out[:, i * cap:(i + 1) * cap] for i in range(len(vals))]

        t_hi, t_lo, t_cnt = to_slots([tok_idx // 64, tok_idx % 64, jnp.ones_like(tok_idx)])
        src = (t_hi * 64.0 + t_lo).astype(jnp.int32)
        src = jnp.where(t_cnt > 0.5, src, tokens)

        def by_pos(table):
            return jnp.roll(table.reshape(ep_size, el, cap), -base, axis=1)

        src_pos = by_pos(src)

        r_hi, r_mid, r_lo = split3(w_router)
        lg = mm(x_tokens, jnp.concatenate([r_hi, r_mid, r_lo], axis=1), ((1,), (0,)))
        logits = lg[:, :experts] + (lg[:, experts:2 * experts] + lg[:, 2 * experts:])
        gate_probs = jax.nn.softmax(logits, axis=-1)
        gate_val = jnp.sum(gate_probs * onehot, axis=-1)
        p_hi, p_mid, p_lo = to_slots(list(split3(gate_val)))
        p_slot = p_hi + (p_mid + p_lo)
        p_recv = lax.all_to_all(by_pos(p_slot), 'ep', 0, 0, tiled=True)
        p_rows = jnp.swapaxes(p_recv, 0, 1).reshape(el, ep_size * cap, 1)
        p_part = lax.ppermute(p_rows[own:].reshape(own, ep_size * cap), 'dp', swap).reshape(own, ep_size * cap, 1)

        def send(rows, q):
            buf = jnp.take(rows, src_pos[:, q].reshape(-1), axis=0, mode='fill', fill_value=0)
            buf = buf.reshape(ep_size, cap, width)
            return lax.all_to_all(buf, 'ep', 0, 0, tiled=True).reshape(ep_size * cap, width)

        def place(q):
            return lax.rem(base + q, el)

        order = []
        for k in range(own):
            order += [own + k, k]
        xs, ys, xp, yp = {}, {}, {}, {}
        for q in order:
            xs[q] = send(x_tokens, q)
            if q >= own:
                xp[q - own] = lax.ppermute(xs[q], 'dp', swap)
            ys[q] = send(grad_y, q)
            if q >= own:
                yp[q - own] = lax.ppermute(ys[q], 'dp', swap)

        g_pos, back, new_in, new_out, stats = {}, {}, [], [], []
        full = None
        for q in order:
            eid = place(q).reshape(1)
            if q >= own:
                dbuf, g_pos[q] = expert_call(eid, xs[q], ys[q], p_rows[q], w_in, w_out)
            else:
                st = (lax.dynamic_index_in_dim(row_in, place(q), 0, keepdims=False)[:, None],
                      lax.dynamic_index_in_dim(col_in, place(q), 0),
                      lax.dynamic_index_in_dim(col_out, place(q), 0, keepdims=False)[:, None],
                      lax.dynamic_index_in_dim(row_out, place(q), 0))
                dbuf, g_pos[q], ni, no, fi, fo, s_in, l_in, s_out, l_out = expert_call(
                    eid, xs[q], ys[q], p_rows[q], w_in, w_out, (xp[q], yp[q], p_part[q]), st, full)
                full = (fi, fo)
                new_in.append(lax.ppermute(ni, 'dp', swap))
                new_out.append(lax.ppermute(no, 'dp', swap))
                stats.append((s_in[:, 0], l_in[0], l_out[0], s_out[:, 0]))
            back[q] = lax.all_to_all(dbuf.reshape(ep_size, cap, width), 'ep', 0, 0, tiled=True).reshape(ep_size * cap, width)

        out_w_in, out_w_out = full
        for k in range(own):
            out_w_in = lax.dynamic_update_index_in_dim(out_w_in, new_in[k], place(own + k), 0)
            out_w_out = lax.dynamic_update_index_in_dim(out_w_out, new_out[k], place(own + k), 0)
        sizes = [s.shape[0] for s in stats[0]]
        mine = jnp.stack([jnp.concatenate(s) for s in stats])
        both = jnp.concatenate([mine, lax.ppermute(mine, 'dp', swap)], axis=0)
        both = jnp.roll(both, base, axis=0)
        out_stats = []
        at = 0
        for size in sizes:
            out_stats.append(both[:, at:at + size])
            at += size

        g_buf = jnp.stack([g_pos[q].reshape(ep_size, cap) for q in range(el)], axis=1)
        g_back = lax.all_to_all(g_buf, 'ep', 0, 0, tiled=True)
        g_slot = jnp.roll(g_back, base, axis=1).reshape(experts, cap)
        g3 = jnp.concatenate(split3(g_slot), axis=0)
        onehot3 = jnp.concatenate([onehot_b] * 3, axis=1)
        g_rows = mm(onehot3, g3, ((1,), (0,)))
        grad_gate = jnp.sum(jnp.where(is_c, g_rows, 0.0), axis=-1)

        route_frac = jnp.mean(onehot, axis=0)
        grad_prob = onehot * grad_gate[:, None] + AUX_COEF * experts * route_frac[None, :] / tokens
        grad_logits = gate_probs * (grad_prob - jnp.sum(gate_probs * grad_prob, axis=-1, keepdims=True))
        l1, l2, l3 = split3(grad_logits)
        gr = mm(x_tokens, jnp.concatenate([l1, l2, l3], axis=1), ((0,), (0,)))
        grad_router = lax.psum(gr[:, :experts] + (gr[:, experts:2 * experts] + gr[:, 2 * experts:]), ('dp', 'ep'))
        lcat = jnp.concatenate([l1, l1, l2, l1, l2, l3], axis=1)
        wcat = jnp.concatenate([r_hi, r_mid, r_hi, r_lo, r_mid, r_hi], axis=1)
        dx_router = mm(lcat, wcat, ((1,), (1,)))

        back_all = jnp.concatenate([back[q] for q in range(el)], axis=0)
        pos_e = lax.rem(expert_id % el - base + el, el)
        back_pos = jnp.where(token_slot >= 0, (pos_e * ep_size + expert_id // el) * cap + token_slot, experts * cap)
        dx_expert = jnp.take(back_all, back_pos, axis=0, mode='fill', fill_value=0)
        grad_x = (dx_expert.astype(F32) + dx_router).astype(BF16)
        new_router, row_router_new, col_router_new = optimizer_step(w_router, grad_router, row_router, col_router)
        return (out_w_in, out_w_out, new_router, out_stats[0], out_stats[1], out_stats[2], out_stats[3], row_router_new, col_router_new, grad_x)

    in_specs = (row_spec, tok_spec, tok_spec, row_spec, full_spec, exp_spec, exp_spec, exp_spec, exp_spec, exp_spec, exp_spec, full_spec, full_spec)
    out_specs = (exp_spec, exp_spec, full_spec, exp_spec, exp_spec, exp_spec, exp_spec, full_spec, full_spec, row_spec)
    return jax.shard_map(local_step, mesh=mesh, in_specs=in_specs, out_specs=out_specs, check_vma=False)
```

```python
import functools
import math

import jax
import jax.numpy as jnp
from jax import lax
from jax.experimental import pallas as pl
from jax.experimental.pallas import tpu as pltpu
from jax.sharding import PartitionSpec as P


OPT_STEP = 2
DECAY_RATE = 1.0 - OPT_STEP ** -0.8
LR_BASE = min(0.01, 1.0 / math.sqrt(OPT_STEP))
AUX_COEF = 0.01
F32 = jnp.float32
BF16 = jnp.bfloat16
OPT_TILE = (640, 1024, 3)
ROWS_TILE = (640, 1536, 2)
G_CHUNK = 64


def kdot(a, b, ca, cb):
    return lax.dot_general(a, b, (((ca,), (cb,)), ((), ())), preferred_element_type=F32)


def adafactor_tile(acc, sub_old, lane_old, sub_new_ref, lane_new_ref, lane_sum, row_is_sub):
    rows, cols = acc.shape
    lane_sum[...] = jnp.zeros_like(lane_sum)

    @pl.loop(0, rows // G_CHUNK)
    def _(i):
        at = pl.ds(pl.multiple_of(i * G_CHUNK, G_CHUNK), G_CHUNK)
        g = acc[at, :]
        v = g * g + 1e-30
        sub_new_ref[at, :] = DECAY_RATE * sub_old[at, :] + (1.0 - DECAY_RATE) * (jnp.sum(v, axis=1, keepdims=True) * (1.0 / cols))
        lane_sum[...] += jnp.sum(v.reshape(G_CHUNK // 8, 8, cols), axis=0)

    lane_new = DECAY_RATE * lane_old[...] + (1.0 - DECAY_RATE) * (jnp.sum(lane_sum[...], axis=0, keepdims=True) * (1.0 / rows))
    lane_new_ref[...] = lane_new
    sub_new = sub_new_ref[...]
    if row_is_sub:
        sub_f = lax.rsqrt(sub_new / (jnp.sum(sub_new, axis=0, keepdims=True) * (1.0 / rows)))
        lane_f = lax.rsqrt(lane_new)
    else:
        lane_f = lax.rsqrt(lane_new / (jnp.sum(lane_new, axis=1, keepdims=True) * (1.0 / cols)))
        sub_f = lax.rsqrt(sub_new)
    return sub_f, lane_f


def expert_kernel(opt, has_back, own_blocks, ids, *refs):
    if has_back:
        at = 5
        refs = refs[:at] + refs[at + 1:]
    if opt:
        (x_ref, y_ref, p_ref, w_in, w_out, sub_in, lane_in, sub_out, lane_out, _, _,
         dbuf, g_out, new_in, new_out, full_in, full_out, sub_in_n, lane_in_n, sub_out_n, lane_out_n,
         w1, w2, sems, h_acc, b_acc, acc_in, acc_out, sub_f, lane_sum) = refs
    else:
        (x_ref, y_ref, p_ref, w_in, w_out, dbuf, g_out, w1, w2, sems, h_acc, b_acc) = refs
    step = pl.program_id(0)
    width, ff = w1.shape
    f_chunk = OPT_TILE[1] if opt else ROWS_TILE[1]
    chunks = ff // f_chunk

    @pl.when(step == 0)
    def _():
        c1 = pltpu.make_async_copy(w_in.at[ids[0]], w1, sems.at[0])
        c2 = pltpu.make_async_copy(w_out.at[ids[0]], w2, sems.at[1])
        c1.start()
        c2.start()
        c1.wait()
        c2.wait()
        if opt:
            acc_in[...] = jnp.zeros_like(acc_in)
            acc_out[...] = jnp.zeros_like(acc_out)

    def body(own):
        rows = p_ref.shape[0]
        p = p_ref[...]
        x = jnp.where(p > 0, x_ref[...].reshape(rows, width).astype(F32), 0.0).astype(BF16)
        dh = (p * y_ref[...].reshape(rows, width).astype(F32)).astype(BF16)
        if opt:
            x_t = x.T
            dh_t = dh.T
        if own:
            h_acc[...] = jnp.zeros_like(h_acc)
            b_acc[...] = jnp.zeros_like(b_acc)

        @pl.loop(0, chunks, unroll=OPT_TILE[2] if opt else ROWS_TILE[2])
        def _(c):
            at = pl.ds(pl.multiple_of(c * f_chunk, f_chunk), f_chunk)
            w1c = w1[:, at]
            w2c = w2[at, :]
            act = jnp.maximum(kdot(x, w1c, 1, 0).astype(BF16), 0)
            ga = kdot(dh, w2c, 1, 1)
            da = jnp.where(act.astype(F32) > 0, ga, 0.0).astype(BF16)
            if own:
                h_acc[...] += kdot(act, w2c, 1, 0)
                b_acc[...] += kdot(da, w1c, 1, 1)
            if opt:
                acc_in[:, at] += kdot(x_t, da, 1, 0)
                acc_out[:, at] += kdot(dh_t, act, 1, 0)

        if own:
            h = h_acc[...].astype(BF16).astype(F32)
            y = y_ref[...].reshape(rows, width).astype(F32)
            g_out[...] = jnp.sum(y * h, axis=1, keepdims=True)
            dbuf[...] = b_acc[...].astype(BF16).reshape(dbuf.shape)

    if opt:
        @pl.when(step < own_blocks)
        def _():
            body(True)

        @pl.when(step >= own_blocks)
        def _():
            body(False)

        @pl.when(step == pl.num_programs(0) - 1)
        def _():
            n = float(width * ff)

            def w_scale(w):
                rows = w.shape[0]

                def one(i, tot):
                    t = w[pl.ds(pl.multiple_of(i * G_CHUNK, G_CHUNK), G_CHUNK), :].astype(F32)
                    return tot + jnp.sum(jnp.sum(t * t, axis=1, keepdims=True), axis=0, keepdims=True)

                tot = lax.fori_loop(0, rows // G_CHUNK, one, jnp.zeros((1, 1), F32))
                return LR_BASE * jnp.maximum(1e-3, jnp.sqrt(tot * (1.0 / n)))

            def u_scale(acc, lane_f):
                def one(i, tot):
                    at = pl.ds(pl.multiple_of(i * G_CHUNK, G_CHUNK), G_CHUNK)
                    u = acc[at, :] * sub_f[at, :] * lane_f
                    acc[at, :] = u
                    return tot + jnp.sum(jnp.sum(u * u, axis=1, keepdims=True), axis=0, keepdims=True)

                tot = lax.fori_loop(0, width // G_CHUNK, one, jnp.zeros((1, 1), F32))
                return 1.0 / jnp.maximum(1.0, jnp.sqrt(tot * (1.0 / n)))

            sf, lf = adafactor_tile(acc_in, sub_in, lane_in, sub_in_n, lane_in_n, lane_sum, True)
            sub_f[...] = sf
            scale = u_scale(acc_in, lf) * w_scale(w1)

            @pl.loop(0, width // G_CHUNK)
            def _(i):
                at = pl.ds(pl.multiple_of(i * G_CHUNK, G_CHUNK), G_CHUNK)
                w1[at, :] = (w1[at, :].astype(F32) - scale * acc_in[at, :]).astype(BF16)

            o1 = pltpu.make_async_copy(w1, new_in, sems.at[0])
            o2 = pltpu.make_async_copy(w1, full_in.at[ids[0]], sems.at[1])
            o1.start()
            o2.start()

            sf2, lf2 = adafactor_tile(acc_out, sub_out, lane_out, sub_out_n, lane_out_n, lane_sum, False)
            sub_f[...] = sf2
            scale2 = u_scale(acc_out, lf2) * w_scale(w2)
            tc = 256

            @pl.loop(0, ff // tc)
            def _(i):
                at = pl.ds(pl.multiple_of(i * tc, tc), tc)
                w2[at, :] = (w2[at, :].astype(F32) - scale2 * acc_out[:, at].T).astype(BF16)

            o3 = pltpu.make_async_copy(w2, new_out, sems.at[2])
            o4 = pltpu.make_async_copy(w2, full_out.at[ids[0]], sems.at[3])
            o3.start()
            o4.start()
            o1.wait()
            o2.wait()
            o3.wait()
            o4.wait()
    else:
        body(True)


def expert_call(ids, x, y, p, w_in, w_out, column, back=None, stats=None, full=None):
    opt = stats is not None
    groups, _, cap, _ = x[0].shape
    el, width, ff = w_in.shape
    row_block = OPT_TILE[0] if opt else ROWS_TILE[0]
    per = row_block // cap
    steps = groups // per
    nb = steps // 2 if opt else steps
    rows = nb * row_block
    if opt:
        at = lambda i, ids: jnp.where(i < nb, ids[1] * nb + i, (1 - ids[1]) * nb + i - nb)
    else:
        at = lambda i, ids: i
    in_specs = [pl.BlockSpec((per, 1, cap, width), lambda i, ids, c=c, w=w: (at(i, ids), c, 0, w)) for _, c, w in (x, y)]
    in_specs.append(pl.BlockSpec((row_block, 1), lambda i, ids: (at(i, ids), 0)))
    args = [x[0], y[0], p]
    out_map = lambda i, ids: (jnp.minimum(i, nb - 1), 0)
    back_map = lambda i, ids: (jnp.minimum(i, nb - 1), column, 0, 0)
    fixed = lambda i, ids: (0, 0)
    any_spec = pl.BlockSpec(memory_space=pl.ANY)
    in_specs += [any_spec, any_spec]
    args += [w_in, w_out]
    out_shape = [jax.ShapeDtypeStruct((rows // cap, el // 2, cap, width), BF16), jax.ShapeDtypeStruct((rows, 1), F32)]
    out_specs = [pl.BlockSpec((per, 1, cap, width), back_map), pl.BlockSpec((row_block, 1), out_map)]
    scratch = [pltpu.VMEM((width, ff), BF16), pltpu.VMEM((ff, width), BF16), pltpu.SemaphoreType.DMA((4,)),
               pltpu.VMEM((row_block, width), F32), pltpu.VMEM((row_block, width), F32)]
    aliases = {}
    if back is not None:
        aliases[1 + len(args)] = 0
        in_specs.append(any_spec)
        args.append(back)
    units = 4
    if opt:
        units = 10
        sub = pl.BlockSpec((width, 1), fixed)
        lane = pl.BlockSpec((1, ff), fixed)
        in_specs += [sub, lane, sub, lane, any_spec, any_spec]
        args += list(stats)
        if full is None:
            full = (jnp.zeros((8, 128), BF16), jnp.zeros((8, 128), BF16))
        else:
            aliases.update({1 + len(args): 4, 2 + len(args): 5})
        args += list(full)
        s, l = jax.ShapeDtypeStruct((width, 1), F32), jax.ShapeDtypeStruct((1, ff), F32)
        out_shape += [jax.ShapeDtypeStruct((width, ff), BF16), jax.ShapeDtypeStruct((ff, width), BF16),
                      jax.ShapeDtypeStruct(w_in.shape, BF16), jax.ShapeDtypeStruct(w_out.shape, BF16), s, l, s, l]
        out_specs += [any_spec] * 4 + [sub, lane, sub, lane]
        scratch += [pltpu.VMEM((width, ff), F32), pltpu.VMEM((width, ff), F32), pltpu.VMEM((width, 1), F32), pltpu.VMEM((8, ff), F32)]
    return pl.pallas_call(
        functools.partial(expert_kernel, opt, back is not None, nb),
        grid_spec=pltpu.PrefetchScalarGridSpec(num_scalar_prefetch=1, grid=(steps,), in_specs=in_specs, out_specs=out_specs, scratch_shapes=scratch),
        out_shape=out_shape,
        input_output_aliases=aliases,
        compiler_params=pltpu.CompilerParams(dimension_semantics=('arbitrary',), vmem_limit_bytes=64_000_000),
        cost_estimate=pl.CostEstimate(flops=units * 2 * rows * width * ff, bytes_accessed=4 * rows * width * 2 + 4 * width * ff, transcendentals=0),
        name='expert_opt' if opt else 'expert_rows',
    )(ids, *args)


def pair_kernel(x, y, _, out):
    width = x.shape[1]
    out[:, :width] = x[...]
    out[:, width:] = y[...]


def pair_rows(x, y, after):
    rows, width = x.shape
    tile = rows // 16
    spec = pl.BlockSpec((tile, width), lambda i: (i, 0))
    return pl.pallas_call(
        pair_kernel,
        grid=(16,),
        in_specs=[spec, spec, pl.BlockSpec(memory_space=pl.ANY)],
        out_specs=pl.BlockSpec((tile, 2 * width), lambda i: (i, 0)),
        out_shape=jax.ShapeDtypeStruct((rows, 2 * width), x.dtype),
        cost_estimate=pl.CostEstimate(flops=rows * width, bytes_accessed=8 * rows * width, transcendentals=0),
        name='pair_rows',
    )(x, y, after)


def optimizer_step(weight, gradient, row_stat, col_stat):
    grad_sq = gradient * gradient + 1e-30
    row_new = DECAY_RATE * row_stat + (1.0 - DECAY_RATE) * jnp.mean(grad_sq, axis=-1)
    col_new = DECAY_RATE * col_stat + (1.0 - DECAY_RATE) * jnp.mean(grad_sq, axis=-2)
    row_norm = row_new / jnp.mean(row_new, axis=-1, keepdims=True)
    update = gradient * lax.rsqrt(row_norm)[..., :, None] * lax.rsqrt(col_new)[..., None, :]
    upd_rms = jnp.sqrt(jnp.mean(update * update, axis=(-2, -1), keepdims=True))
    update = update / jnp.maximum(1.0, upd_rms)
    w_full = weight.astype(F32)
    w_rms = jnp.sqrt(jnp.mean(w_full * w_full, axis=(-2, -1), keepdims=True))
    new_weight = w_full - LR_BASE * jnp.maximum(1e-3, w_rms) * update
    return new_weight, row_new, col_new


def split3(value):
    hi = lax.reduce_precision(value, 8, 7)
    rest = value - hi
    mid = lax.reduce_precision(rest, 8, 7)
    lo = rest - mid
    return hi.astype(BF16), mid.astype(BF16), lo.astype(BF16)


def mm(a, b, dims):
    return lax.dot_general(a, b, (dims, ((), ())), preferred_element_type=F32)


def solution(mesh):
    ep_size = mesh.shape['ep']
    dp_size = mesh.shape['dp']
    tok_spec = P(('dp', 'ep'))
    row_spec = P(('dp', 'ep'), None)
    exp_spec = P('ep')
    full_spec = P()
    swap = [(i, (i + 1) % dp_size) for i in range(dp_size)]

    def step_body(x_tokens, expert_id, token_slot, grad_y, w_router, w_in, w_out, row_in, col_in, row_out, col_out, row_router, col_router):
        tokens, width = x_tokens.shape
        el = w_in.shape[0]
        experts = w_router.shape[1]
        cap = 5 * tokens // (4 * experts)
        own = el // dp_size
        zi = lax.axis_index('dp')
        base = own * zi

        is_e = expert_id[:, None] == jnp.arange(experts)[None, :]
        onehot = is_e.astype(F32)
        onehot_b = is_e.astype(BF16)
        is_c = token_slot[:, None] == jnp.arange(cap)[None, :]
        tok_idx = jnp.arange(tokens, dtype=jnp.int32)

        def to_slots(vals):
            cols = jnp.concatenate([jnp.where(is_c, v.astype(BF16)[:, None], jnp.zeros((), BF16)) for v in vals], axis=1)
            out = mm(onehot_b, cols, ((0,), (0,)))
            return [out[:, i * cap:(i + 1) * cap] for i in range(len(vals))]

        t_hi, t_lo = to_slots([tok_idx // 64, tok_idx % 64])
        src = (t_hi * 64.0 + t_lo).astype(jnp.int32).reshape(ep_size, dp_size, own, cap)

        def rows_of(table, index):
            return jnp.take(table, index.reshape(-1), axis=0, mode='clip').reshape(index.shape + table.shape[1:])

        def at_dp(table, i):
            return lax.dynamic_index_in_dim(table, i, 1, keepdims=False)

        def to_owners(table, k):
            buf = rows_of(table, jnp.swapaxes(src[:, :, k], 0, 1))
            buf = buf.reshape(dp_size * ep_size, 1, cap, -1)
            return lax.all_to_all(buf, ('dp', 'ep'), 0, 0, tiled=True), buf

        x_first, _ = to_owners(x_tokens, 0)
        y_first, y_buf = to_owners(grad_y, 0)
        xy_tok = pair_rows(x_tokens, grad_y, y_buf)
        xy_own = [None] + [to_owners(xy_tok, k)[0] for k in range(1, own)]
        buf = rows_of(xy_tok, at_dp(src, 1 - zi))
        xy_non = lax.all_to_all(buf, 'ep', 0, 0, tiled=True)

        r_hi, r_mid, r_lo = split3(w_router)
        lg = mm(x_tokens, jnp.concatenate([r_hi, r_mid, r_lo], axis=1), ((1,), (0,)))
        logits = lg[:, :experts] + (lg[:, experts:2 * experts] + lg[:, 2 * experts:])
        gate_probs = jax.nn.softmax(logits, axis=-1)
        gate_val = jnp.sum(gate_probs * onehot, axis=-1)
        p_hi, p_mid, p_lo = to_slots(list(split3(gate_val)))
        p_slot = (p_hi + (p_mid + p_lo)).reshape(ep_size, dp_size, own, cap)
        p_all = jnp.broadcast_to(p_slot[None], (dp_size,) + p_slot.shape).reshape(dp_size * ep_size, dp_size, own, cap)
        p_all = lax.all_to_all(p_all, ('dp', 'ep'), 0, 0, tiled=True)
        p_own = lax.dynamic_index_in_dim(p_all, zi, 1, keepdims=False)
        p_non = lax.dynamic_slice_in_dim(lax.dynamic_index_in_dim(p_all, 1 - zi, 1, keepdims=False), zi * ep_size, ep_size, 0)

        def stat(table, e):
            return lax.dynamic_index_in_dim(table, e, 0)

        g_pos, new_in, new_out, stats = [], [], [], []
        full = back_a = back_b = None
        for k in range(own):
            e = base + k
            ids = jnp.stack([e, zi])
            st = (stat(row_in, e).reshape(width, 1), stat(col_in, e), stat(col_out, e).reshape(width, 1), stat(row_out, e))
            back_b, g, ni, no, fi, fo, s_in, l_in, s_out, l_out = expert_call(ids, *(((xy_own[k], 0, 0), (xy_own[k], 0, 1)) if k else ((x_first, 0, 0), (y_first, 0, 0))), p_own[:, k].reshape(-1, 1), w_in, w_out, k, back=back_b, stats=st, full=full)
            full = (fi, fo)
            new_in.append(lax.ppermute(ni, 'dp', swap))
            new_out.append(lax.ppermute(no, 'dp', swap))
            stats.append((s_in[:, 0], l_in[0], l_out[0], s_out[:, 0]))
            g_pos.append(g)
        last = stats[-1][0]
        for k in range(own):
            e = lax.rem(base + own + k, el)
            ids, _ = lax.optimization_barrier((jnp.stack([e, zi]), last))
            back_a, g = expert_call(ids, (xy_non, k, 0), (xy_non, k, 1), p_non[:, k].reshape(-1, 1), w_in, w_out, k, back=back_a)
            last = g
            g_pos.append(g)
        back_b = lax.all_to_all(back_b, 'ep', 0, 0, tiled=True)
        back_a = lax.all_to_all(back_a, 'ep', 0, 0, tiled=True)

        out_w_in, out_w_out = full
        for k in range(own):
            e = lax.rem(base + own + k, el)
            out_w_in = lax.dynamic_update_index_in_dim(out_w_in, new_in[k], e, 0)
            out_w_out = lax.dynamic_update_index_in_dim(out_w_out, new_out[k], e, 0)
        sizes = [s.shape[0] for s in stats[0]]
        mine = jnp.stack([jnp.concatenate(s) for s in stats])
        both = jnp.concatenate([mine, lax.ppermute(mine, 'dp', swap)], axis=0)
        both = jnp.roll(both, base, axis=0)
        out_stats = []
        at = 0
        for size in sizes:
            out_stats.append(both[:, at:at + size])
            at += size

        g_buf = jnp.stack([g.reshape(ep_size, cap) for g in g_pos], axis=1)
        g_back = lax.all_to_all(g_buf, 'ep', 0, 0, tiled=True)
        g_slot = jnp.roll(g_back, base, axis=1).reshape(experts, cap)
        g3 = jnp.concatenate(split3(g_slot), axis=0)
        onehot3 = jnp.concatenate([onehot_b] * 3, axis=1)
        g_rows = mm(onehot3, g3, ((1,), (0,)))
        grad_gate = jnp.sum(jnp.where(is_c, g_rows, 0.0), axis=-1)

        route_frac = jnp.mean(onehot, axis=0)
        grad_prob = onehot * grad_gate[:, None] + AUX_COEF * experts * route_frac[None, :] / tokens
        grad_logits = gate_probs * (grad_prob - jnp.sum(gate_probs * grad_prob, axis=-1, keepdims=True))
        l1, l2, l3 = split3(grad_logits)
        gr = mm(x_tokens, jnp.concatenate([l1, l2, l3], axis=1), ((0,), (0,)))
        grad_router = lax.psum(gr[:, :experts] + (gr[:, experts:2 * experts] + gr[:, 2 * experts:]), ('dp', 'ep'))
        lcat = jnp.concatenate([l1, l1, l2, l1, l2, l3], axis=1)
        wcat = jnp.concatenate([r_hi, r_mid, r_hi, r_lo, r_mid, r_hi], axis=1)
        dx_router = mm(lcat, wcat, ((1,), (1,)))

        slot_at = (expert_id // el * own + expert_id % own) * cap + token_slot
        mine_e = expert_id % el // own == zi
        nowhere = ep_size * own * cap

        def rows_back(table, here):
            index = jnp.where((token_slot >= 0) & here, slot_at, nowhere)
            return jnp.take(table.reshape(nowhere, width), index, axis=0, mode='fill', fill_value=0)

        dx_b = rows_back(back_b, mine_e)
        dx_a = rows_back(back_a, jnp.logical_not(mine_e))
        dx_expert = dx_b + dx_a
        grad_x = (dx_expert.astype(F32) + dx_router).astype(BF16)
        new_router, row_router_new, col_router_new = optimizer_step(w_router, grad_router, row_router, col_router)
        return (out_w_in, out_w_out, new_router, out_stats[0], out_stats[1], out_stats[2], out_stats[3], row_router_new, col_router_new, grad_x)

    in_specs = (row_spec, tok_spec, tok_spec, row_spec, full_spec, exp_spec, exp_spec, exp_spec, exp_spec, exp_spec, exp_spec, full_spec, full_spec)
    out_specs = (exp_spec, exp_spec, full_spec, exp_spec, exp_spec, exp_spec, exp_spec, full_spec, full_spec, row_spec)
    return jax.shard_map(step_body, mesh=mesh, in_specs=in_specs, out_specs=out_specs, check_vma=False)
```

```python
import functools
import math

import jax
import jax.numpy as jnp
from jax import lax
from jax.experimental import pallas as pl
from jax.experimental.pallas import tpu as pltpu
from jax.sharding import PartitionSpec as P


OPT_STEP = 2
DECAY_RATE = 1.0 - OPT_STEP ** -0.8
LR_BASE = min(0.01, 1.0 / math.sqrt(OPT_STEP))
AUX_COEF = 0.01
F32 = jnp.float32
BF16 = jnp.bfloat16
ROW_BLOCK = 640
FORMS = ((208, 1024, 3), (256, 512, 1), (320, 512, 1))
G_CHUNK = 64


def kdot(a, b, ca, cb):
    return lax.dot_general(a, b, (((ca,), (cb,)), ((), ())), preferred_element_type=F32)


def adafactor_tile(acc, sub_old, lane_old, sub_new_ref, lane_new_ref, lane_sum, row_is_sub):
    rows, cols = acc.shape
    lane_sum[...] = jnp.zeros_like(lane_sum)

    @pl.loop(0, rows // G_CHUNK)
    def _(i):
        at = pl.ds(pl.multiple_of(i * G_CHUNK, G_CHUNK), G_CHUNK)
        g = acc[at, :]
        v = g * g + 1e-30
        sub_new_ref[at, :] = DECAY_RATE * sub_old[at, :] + (1.0 - DECAY_RATE) * (jnp.sum(v, axis=1, keepdims=True) * (1.0 / cols))
        lane_sum[...] += jnp.sum(v.reshape(G_CHUNK // 8, 8, cols), axis=0)

    lane_new = DECAY_RATE * lane_old[...] + (1.0 - DECAY_RATE) * (jnp.sum(lane_sum[...], axis=0, keepdims=True) * (1.0 / rows))
    lane_new_ref[...] = lane_new
    sub_new = sub_new_ref[...]
    if row_is_sub:
        sub_f = lax.rsqrt(sub_new / (jnp.sum(sub_new, axis=0, keepdims=True) * (1.0 / rows)))
        lane_f = lax.rsqrt(lane_new)
    else:
        lane_f = lax.rsqrt(lane_new / (jnp.sum(lane_new, axis=1, keepdims=True) * (1.0 / cols)))
        sub_f = lax.rsqrt(sub_new)
    return sub_f, lane_f


def expert_kernel(opt, has_back, own_blocks, ids, *refs):
    if has_back:
        at = 5
        refs = refs[:at] + refs[at + 1:]
    if opt:
        (x_ref, y_ref, p_ref, w_in, w_out, sub_in, lane_in, sub_out, lane_out, _, _,
         dbuf, g_out, new_in, new_out, full_in, full_out, sub_in_n, lane_in_n, sub_out_n, lane_out_n,
         w1, w2, sems, h_acc, b_acc, acc_in, acc_out, sub_f, lane_sum) = refs
    else:
        (x_ref, y_ref, p_ref, w_in, w_out, dbuf, g_out, w1, w2, sems, h_acc, b_acc) = refs
    step = pl.program_id(0)
    width, ff = w1.shape


    @pl.when(step == 0)
    def _():
        c1 = pltpu.make_async_copy(w_in.at[ids[0]], w1, sems.at[0])
        c2 = pltpu.make_async_copy(w_out.at[ids[0]], w2, sems.at[1])
        c1.start()
        c2.start()
        c1.wait()
        c2.wait()
        if opt:
            acc_in[...] = jnp.zeros_like(acc_in)
            acc_out[...] = jnp.zeros_like(acc_out)

    def body(own, live, f_chunk, unroll):
        per, _, cap, _ = x_ref.shape
        rows = per * live
        p = p_ref[...].reshape(per, cap, 1)[:, :live].reshape(rows, 1)
        x = jnp.where(p > 0, x_ref[:, 0, :live, :].reshape(rows, width).astype(F32), 0.0).astype(BF16)
        dh = (p * y_ref[:, 0, :live, :].reshape(rows, width).astype(F32)).astype(BF16)
        if opt:
            x_t = x.T
            dh_t = dh.T
        if own:
            h_acc[:rows] = jnp.zeros((rows, width), F32)
            b_acc[:rows] = jnp.zeros((rows, width), F32)

        @pl.loop(0, ff // f_chunk, unroll=unroll)
        def _(c):
            at = pl.ds(pl.multiple_of(c * f_chunk, f_chunk), f_chunk)
            w1c = w1[:, at]
            w2c = w2[at, :]
            act = jnp.maximum(kdot(x, w1c, 1, 0).astype(BF16), 0)
            ga = kdot(dh, w2c, 1, 1)
            da = jnp.where(act.astype(F32) > 0, ga, 0.0).astype(BF16)
            if own:
                h_acc[:rows] += kdot(act, w2c, 1, 0)
                b_acc[:rows] += kdot(da, w1c, 1, 1)
            if opt:
                acc_in[:, at] += kdot(x_t, da, 1, 0)
                acc_out[:, at] += kdot(dh_t, act, 1, 0)

        if own:
            h = h_acc[:rows].astype(BF16).astype(F32)
            y = y_ref[:, 0, :live, :].reshape(rows, width).astype(F32)
            g = jnp.sum(y * h, axis=1, keepdims=True).reshape(per, live, 1)
            db = b_acc[:rows].astype(BF16).reshape(per, live, width)
            for i in range(per):
                g_out[i * cap:i * cap + live] = g[i]
                dbuf[i, 0, :live, :] = db[i]
                if live < cap:
                    g_out[i * cap + live:(i + 1) * cap] = jnp.zeros((cap - live, 1), F32)
                    dbuf[i, 0, live:, :] = jnp.zeros((cap - live, width), BF16)

    def forms(own):
        low = -1
        for live, f_chunk, unroll in FORMS:
            used = ids[2 + step]

            @pl.when((used > low) & (used <= live))
            def _(live=live, f_chunk=f_chunk, unroll=unroll):
                body(own, live, f_chunk, unroll)

            low = live

    if opt:
        @pl.when(step < own_blocks)
        def _():
            forms(True)

        @pl.when(step >= own_blocks)
        def _():
            forms(False)

        @pl.when(step == pl.num_programs(0) - 1)
        def _():
            n = float(width * ff)

            def w_scale(w):
                rows = w.shape[0]

                def one(i, tot):
                    t = w[pl.ds(pl.multiple_of(i * G_CHUNK, G_CHUNK), G_CHUNK), :].astype(F32)
                    return tot + jnp.sum(jnp.sum(t * t, axis=1, keepdims=True), axis=0, keepdims=True)

                tot = lax.fori_loop(0, rows // G_CHUNK, one, jnp.zeros((1, 1), F32))
                return LR_BASE * jnp.maximum(1e-3, jnp.sqrt(tot * (1.0 / n)))

            def u_scale(acc, lane_f):
                def one(i, tot):
                    at = pl.ds(pl.multiple_of(i * G_CHUNK, G_CHUNK), G_CHUNK)
                    u = acc[at, :] * sub_f[at, :] * lane_f
                    acc[at, :] = u
                    return tot + jnp.sum(jnp.sum(u * u, axis=1, keepdims=True), axis=0, keepdims=True)

                tot = lax.fori_loop(0, width // G_CHUNK, one, jnp.zeros((1, 1), F32))
                return 1.0 / jnp.maximum(1.0, jnp.sqrt(tot * (1.0 / n)))

            sf, lf = adafactor_tile(acc_in, sub_in, lane_in, sub_in_n, lane_in_n, lane_sum, True)
            sub_f[...] = sf
            scale = u_scale(acc_in, lf) * w_scale(w1)

            @pl.loop(0, width // G_CHUNK)
            def _(i):
                at = pl.ds(pl.multiple_of(i * G_CHUNK, G_CHUNK), G_CHUNK)
                w1[at, :] = (w1[at, :].astype(F32) - scale * acc_in[at, :]).astype(BF16)

            o1 = pltpu.make_async_copy(w1, new_in, sems.at[0])
            o2 = pltpu.make_async_copy(w1, full_in.at[ids[0]], sems.at[1])
            o1.start()
            o2.start()

            sf2, lf2 = adafactor_tile(acc_out, sub_out, lane_out, sub_out_n, lane_out_n, lane_sum, False)
            sub_f[...] = sf2
            scale2 = u_scale(acc_out, lf2) * w_scale(w2)
            tc = 256

            @pl.loop(0, ff // tc)
            def _(i):
                at = pl.ds(pl.multiple_of(i * tc, tc), tc)
                w2[at, :] = (w2[at, :].astype(F32) - scale2 * acc_out[:, at].T).astype(BF16)

            o3 = pltpu.make_async_copy(w2, new_out, sems.at[2])
            o4 = pltpu.make_async_copy(w2, full_out.at[ids[0]], sems.at[3])
            o3.start()
            o4.start()
            o1.wait()
            o2.wait()
            o3.wait()
            o4.wait()
    else:
        forms(True)


def expert_call(ids, x, y, p, w_in, w_out, column, back=None, stats=None, full=None):
    opt = stats is not None
    groups, _, cap, _ = x[0].shape
    el, width, ff = w_in.shape
    row_block = ROW_BLOCK
    per = row_block // cap
    steps = groups // per
    nb = steps // 2 if opt else steps
    rows = nb * row_block
    if opt:
        at = lambda i, ids: jnp.where(i < nb, ids[1] * nb + i, (1 - ids[1]) * nb + i - nb)
    else:
        at = lambda i, ids: i
    used = jnp.max(jnp.where(p.reshape(steps, per, cap) > 0, jnp.arange(1, cap + 1, dtype=jnp.int32), 0), axis=(1, 2))
    if opt:
        used = jnp.roll(used, -nb * ids[1])
    ids = jnp.concatenate([ids, used])
    in_specs = [pl.BlockSpec((per, 1, cap, width), lambda i, ids, c=c, w=w: (at(i, ids), c, 0, w)) for _, c, w in (x, y)]
    in_specs.append(pl.BlockSpec((row_block, 1), lambda i, ids: (at(i, ids), 0)))
    args = [x[0], y[0], p]
    out_map = lambda i, ids: (jnp.minimum(i, nb - 1), 0)
    back_map = lambda i, ids: (jnp.minimum(i, nb - 1), column, 0, 0)
    fixed = lambda i, ids: (0, 0)
    any_spec = pl.BlockSpec(memory_space=pl.ANY)
    in_specs += [any_spec, any_spec]
    args += [w_in, w_out]
    out_shape = [jax.ShapeDtypeStruct((rows // cap, el // 2, cap, width), BF16), jax.ShapeDtypeStruct((rows, 1), F32)]
    out_specs = [pl.BlockSpec((per, 1, cap, width), back_map), pl.BlockSpec((row_block, 1), out_map)]
    scratch = [pltpu.VMEM((width, ff), BF16), pltpu.VMEM((ff, width), BF16), pltpu.SemaphoreType.DMA((4,)),
               pltpu.VMEM((row_block, width), F32), pltpu.VMEM((row_block, width), F32)]
    aliases = {}
    if back is not None:
        aliases[1 + len(args)] = 0
        in_specs.append(any_spec)
        args.append(back)
    units = 4
    if opt:
        units = 10
        sub = pl.BlockSpec((width, 1), fixed)
        lane = pl.BlockSpec((1, ff), fixed)
        in_specs += [sub, lane, sub, lane, any_spec, any_spec]
        args += list(stats)
        if full is None:
            full = (jnp.zeros((8, 128), BF16), jnp.zeros((8, 128), BF16))
        else:
            aliases.update({1 + len(args): 4, 2 + len(args): 5})
        args += list(full)
        s, l = jax.ShapeDtypeStruct((width, 1), F32), jax.ShapeDtypeStruct((1, ff), F32)
        out_shape += [jax.ShapeDtypeStruct((width, ff), BF16), jax.ShapeDtypeStruct((ff, width), BF16),
                      jax.ShapeDtypeStruct(w_in.shape, BF16), jax.ShapeDtypeStruct(w_out.shape, BF16), s, l, s, l]
        out_specs += [any_spec] * 4 + [sub, lane, sub, lane]
        scratch += [pltpu.VMEM((width, ff), F32), pltpu.VMEM((width, ff), F32), pltpu.VMEM((width, 1), F32), pltpu.VMEM((8, ff), F32)]
    return pl.pallas_call(
        functools.partial(expert_kernel, opt, back is not None, nb),
        grid_spec=pltpu.PrefetchScalarGridSpec(num_scalar_prefetch=1, grid=(steps,), in_specs=in_specs, out_specs=out_specs, scratch_shapes=scratch),
        out_shape=out_shape,
        input_output_aliases=aliases,
        compiler_params=pltpu.CompilerParams(dimension_semantics=('arbitrary',), vmem_limit_bytes=64_000_000),
        cost_estimate=pl.CostEstimate(flops=units * 2 * rows * width * ff, bytes_accessed=4 * rows * width * 2 + 4 * width * ff, transcendentals=0),
        name='expert_opt' if opt else 'expert_rows',
    )(ids, *args)


def pair_kernel(x, y, _, out):
    width = x.shape[1]
    out[:, :width] = x[...]
    out[:, width:] = y[...]


def pair_rows(x, y, after):
    rows, width = x.shape
    tile = rows // 16
    spec = pl.BlockSpec((tile, width), lambda i: (i, 0))
    return pl.pallas_call(
        pair_kernel,
        grid=(16,),
        in_specs=[spec, spec, pl.BlockSpec(memory_space=pl.ANY)],
        out_specs=pl.BlockSpec((tile, 2 * width), lambda i: (i, 0)),
        out_shape=jax.ShapeDtypeStruct((rows, 2 * width), x.dtype),
        cost_estimate=pl.CostEstimate(flops=rows * width, bytes_accessed=8 * rows * width, transcendentals=0),
        name='pair_rows',
    )(x, y, after)


def optimizer_step(weight, gradient, row_stat, col_stat):
    grad_sq = gradient * gradient + 1e-30
    row_new = DECAY_RATE * row_stat + (1.0 - DECAY_RATE) * jnp.mean(grad_sq, axis=-1)
    col_new = DECAY_RATE * col_stat + (1.0 - DECAY_RATE) * jnp.mean(grad_sq, axis=-2)
    row_norm = row_new / jnp.mean(row_new, axis=-1, keepdims=True)
    update = gradient * lax.rsqrt(row_norm)[..., :, None] * lax.rsqrt(col_new)[..., None, :]
    upd_rms = jnp.sqrt(jnp.mean(update * update, axis=(-2, -1), keepdims=True))
    update = update / jnp.maximum(1.0, upd_rms)
    w_full = weight.astype(F32)
    w_rms = jnp.sqrt(jnp.mean(w_full * w_full, axis=(-2, -1), keepdims=True))
    new_weight = w_full - LR_BASE * jnp.maximum(1e-3, w_rms) * update
    return new_weight, row_new, col_new


def split3(value):
    hi = lax.reduce_precision(value, 8, 7)
    rest = value - hi
    mid = lax.reduce_precision(rest, 8, 7)
    lo = rest - mid
    return hi.astype(BF16), mid.astype(BF16), lo.astype(BF16)


def mm(a, b, dims):
    return lax.dot_general(a, b, (dims, ((), ())), preferred_element_type=F32)


def solution(mesh):
    ep_size = mesh.shape['ep']
    dp_size = mesh.shape['dp']
    tok_spec = P(('dp', 'ep'))
    row_spec = P(('dp', 'ep'), None)
    exp_spec = P('ep')
    full_spec = P()
    swap = [(i, (i + 1) % dp_size) for i in range(dp_size)]

    def step_body(x_tokens, expert_id, token_slot, grad_y, w_router, w_in, w_out, row_in, col_in, row_out, col_out, row_router, col_router):
        tokens, width = x_tokens.shape
        el = w_in.shape[0]
        experts = w_router.shape[1]
        cap = 5 * tokens // (4 * experts)
        own = el // dp_size
        zi = lax.axis_index('dp')
        base = own * zi

        is_e = expert_id[:, None] == jnp.arange(experts)[None, :]
        onehot = is_e.astype(F32)
        onehot_b = is_e.astype(BF16)
        is_c = token_slot[:, None] == jnp.arange(cap)[None, :]
        tok_idx = jnp.arange(tokens, dtype=jnp.int32)

        def to_slots(vals, is_c):
            cols = jnp.concatenate([jnp.where(is_c, v.astype(BF16)[:, None], jnp.zeros((), BF16)) for v in vals], axis=1)
            out = mm(onehot_b, cols, ((0,), (0,)))
            return [out[:, i * cap:(i + 1) * cap] for i in range(len(vals))]

        t_hi, t_lo = to_slots([tok_idx // 64, tok_idx % 64], is_c)
        src = (t_hi * 64.0 + t_lo).astype(jnp.int32).reshape(ep_size, dp_size, own, cap)

        def rows_of(table, index):
            return jnp.take(table, index.reshape(-1), axis=0, mode='clip').reshape(index.shape + table.shape[1:])

        def at_dp(table, i):
            return lax.dynamic_index_in_dim(table, i, 1, keepdims=False)

        def to_owners(table, k):
            buf = rows_of(table, jnp.swapaxes(src[:, :, k], 0, 1))
            buf = buf.reshape(dp_size * ep_size, 1, cap, -1)
            return lax.all_to_all(buf, ('dp', 'ep'), 0, 0, tiled=True), buf

        x_first, x_buf = to_owners(x_tokens, 0)
        y_first, y_buf = to_owners(grad_y, 0)
        xy_tok = pair_rows(x_tokens, grad_y, y_buf)
        xy_own = [None] + [to_owners(xy_tok, k)[0] for k in range(1, own)]
        buf = rows_of(xy_tok, at_dp(src, 1 - zi))
        xy_non = lax.all_to_all(buf, 'ep', 0, 0, tiled=True)

        r_hi, r_mid, r_lo = split3(w_router)
        lg = mm(x_tokens, jnp.concatenate([r_hi, r_mid, r_lo], axis=1), ((1,), (0,)))
        logits = lg[:, :experts] + (lg[:, experts:2 * experts] + lg[:, 2 * experts:])
        gate_probs = jax.nn.softmax(logits, axis=-1)
        gate_val = jnp.sum(gate_probs * onehot, axis=-1)
        slot_later, _ = lax.optimization_barrier((token_slot, x_buf))
        p_hi, p_mid, p_lo = to_slots(list(split3(gate_val)), slot_later[:, None] == jnp.arange(cap)[None, :])
        p_slot = (p_hi + (p_mid + p_lo)).reshape(ep_size, dp_size, own, cap)
        p_all = jnp.broadcast_to(p_slot[None], (dp_size,) + p_slot.shape).reshape(dp_size * ep_size, dp_size, own, cap)
        p_all = lax.all_to_all(p_all, ('dp', 'ep'), 0, 0, tiled=True)
        p_own = lax.dynamic_index_in_dim(p_all, zi, 1, keepdims=False)
        p_non = lax.dynamic_slice_in_dim(lax.dynamic_index_in_dim(p_all, 1 - zi, 1, keepdims=False), zi * ep_size, ep_size, 0)

        p_rows = []
        for k in range(own):
            p_rows.append(p_own[:, k].reshape(-1, 1))
        for k in range(own):
            p_rows.append(p_non[:, k].reshape(-1, 1))

        def stat(table, e):
            return lax.dynamic_index_in_dim(table, e, 0)

        g_pos, new_in, new_out, stats = [], [], [], []
        full = back_a = back_b = None
        for k in range(own):
            e = base + k
            ids = jnp.stack([e, zi])
            st = (stat(row_in, e).reshape(width, 1), stat(col_in, e), stat(col_out, e).reshape(width, 1), stat(row_out, e))
            back_b, g, ni, no, fi, fo, s_in, l_in, s_out, l_out = expert_call(ids, *(((xy_own[k], 0, 0), (xy_own[k], 0, 1)) if k else ((x_first, 0, 0), (y_first, 0, 0))), p_rows[k], w_in, w_out, k, back=back_b, stats=st, full=full)
            full = (fi, fo)
            new_in.append(lax.ppermute(ni, 'dp', swap))
            new_out.append(lax.ppermute(no, 'dp', swap))
            stats.append((s_in[:, 0], l_in[0], l_out[0], s_out[:, 0]))
            g_pos.append(g)
        last = stats[-1][0]
        for k in range(own):
            e = lax.rem(base + own + k, el)
            ids, _ = lax.optimization_barrier((jnp.stack([e, zi]), last))
            back_a, g = expert_call(ids, (xy_non, k, 0), (xy_non, k, 1), p_rows[own + k], w_in, w_out, k, back=back_a)
            last = g
            g_pos.append(g)
        back_b = lax.all_to_all(back_b, 'ep', 0, 0, tiled=True)
        back_a = lax.all_to_all(back_a, 'ep', 0, 0, tiled=True)

        out_w_in, out_w_out = full
        for k in range(own):
            e = lax.rem(base + own + k, el)
            out_w_in = lax.dynamic_update_index_in_dim(out_w_in, new_in[k], e, 0)
            out_w_out = lax.dynamic_update_index_in_dim(out_w_out, new_out[k], e, 0)
        sizes = [s.shape[0] for s in stats[0]]
        mine = jnp.stack([jnp.concatenate(s) for s in stats])
        both = jnp.concatenate([mine, lax.ppermute(mine, 'dp', swap)], axis=0)
        both = jnp.roll(both, base, axis=0)
        out_stats = []
        at = 0
        for size in sizes:
            out_stats.append(both[:, at:at + size])
            at += size

        g_buf = jnp.stack([g.reshape(ep_size, cap) for g in g_pos], axis=1)
        g_back = lax.all_to_all(g_buf, 'ep', 0, 0, tiled=True)
        g_slot = jnp.roll(g_back, base, axis=1).reshape(experts, cap)
        g3 = jnp.concatenate(split3(g_slot), axis=0)
        onehot3 = jnp.concatenate([onehot_b] * 3, axis=1)
        g_rows = mm(onehot3, g3, ((1,), (0,)))
        grad_gate = jnp.sum(jnp.where(is_c, g_rows, 0.0), axis=-1)

        route_frac = jnp.mean(onehot, axis=0)
        grad_prob = onehot * grad_gate[:, None] + AUX_COEF * experts * route_frac[None, :] / tokens
        grad_logits = gate_probs * (grad_prob - jnp.sum(gate_probs * grad_prob, axis=-1, keepdims=True))
        l1, l2, l3 = split3(grad_logits)
        gr = mm(x_tokens, jnp.concatenate([l1, l2, l3], axis=1), ((0,), (0,)))
        grad_router = lax.psum(gr[:, :experts] + (gr[:, experts:2 * experts] + gr[:, 2 * experts:]), ('dp', 'ep'))
        lcat = jnp.concatenate([l1, l1, l2, l1, l2, l3], axis=1)
        wcat = jnp.concatenate([r_hi, r_mid, r_hi, r_lo, r_mid, r_hi], axis=1)
        dx_router = mm(lcat, wcat, ((1,), (1,)))

        slot_at = (expert_id // el * own + expert_id % own) * cap + token_slot
        mine_e = expert_id % el // own == zi
        nowhere = ep_size * own * cap

        def rows_back(table, here):
            index = jnp.where((token_slot >= 0) & here, slot_at, nowhere)
            return jnp.take(table.reshape(nowhere, width), index, axis=0, mode='fill', fill_value=0)

        dx_b = rows_back(back_b, mine_e)
        dx_a = rows_back(back_a, jnp.logical_not(mine_e))
        dx_expert = dx_b + dx_a
        grad_x = (dx_expert.astype(F32) + dx_router).astype(BF16)
        new_router, row_router_new, col_router_new = optimizer_step(w_router, grad_router, row_router, col_router)
        return (out_w_in, out_w_out, new_router, out_stats[0], out_stats[1], out_stats[2], out_stats[3], row_router_new, col_router_new, grad_x)

    in_specs = (row_spec, tok_spec, tok_spec, row_spec, full_spec, exp_spec, exp_spec, exp_spec, exp_spec, exp_spec, exp_spec, full_spec, full_spec)
    out_specs = (exp_spec, exp_spec, full_spec, exp_spec, exp_spec, exp_spec, exp_spec, full_spec, full_spec, row_spec)
    return jax.shard_map(step_body, mesh=mesh, in_specs=in_specs, out_specs=out_specs, check_vma=False)
```
